1024 devices in a mesh: gx: 4 (over z_hi, core), gy: 16 (over z_lo), gz: 16 (over y, x).
Axes of the slice: x: 4, y: 4, z: 32 (z_hi: 2, z_lo: 16; z = z_hi * 16 + z_lo), core: 2. Of those that a mesh axis runs over, the one named last changes fastest.
Arguments:
- positions: float32 [4, 16, 16, 2, 3, 128], P('gx', 'gy', 'gz'), may hold values from 0 to 48, as said below
- features: bfloat16 [4, 16, 16, 2, 128, 128], P('gx', 'gy', 'gz'), may hold values from -6 to 6
- counts: int32 [4, 16, 16, 2], P('gx', 'gy', 'gz'), may hold values from 0 to 128, as said below
- neighbours: int32 [4, 16, 16, 2, 8], P('gx', 'gy', 'gz'), may hold values from -1 to 53, as said below
- mix_weight: bfloat16 [1024, 128], replicated, may hold values from -0.1875 to 0.1875
- readout: float32 [128], replicated, may hold values from -4 to 4
- radial_rates: float32 [4], replicated, may hold values from 0.03 to 0.6
Outputs:
- forces: float32 [4, 16, 16, 2, 3, 128], P('gx', 'gy', 'gz')
- feature_grads: float32 [4, 16, 16, 2, 128, 128], P('gx', 'gy', 'gz')
The draws below stay inside these ranges and needn't reach their ends.
Inputs may be any that keep to these rules, and one draw needn't show every extreme that they name: The atoms of a tile fill its first counts slots; a count of 0 marks a tile slot that its device doesn't own; every draw has a tile with 128 atoms. neighbours[.., t, s] names a tile of the device's neighbourhood as ((dx + 1) * 9 + (dy + 1) * 3 + (dz + 1)) * 2 + u, dx, dy, dz in -1..1 being the device offsets along gx, gy, gz and u the tile slot; slot 0 names tile t itself, every other used slot names a tile with one or more atoms, the entries of a row differ, and -1 marks unused slots, which come after the used ones. `positions`: the atoms of device (a, b, c) lie in the cube of side 3 whose lowest corner is 3 (a, b, c).
All inputs are finite; a program needn't handle non-finite values.
Results may differ from the reference program's by a relative error of at most 0.0008.
Values may be sent and summed in bfloat16 or wider, within the bound.
A program may use at most 32 MiB of HBM per device.

```python
import math
import jax
import jax.numpy as jnp
from jax import lax

ATOMS = 128
CH = 128
RAD = 4
NBR = 8
TPD = 2
N_GX = 4
N_GY = 16
N_GZ = 16


box_side = 3.0


def draw_positions(key, part):
    full_shape = (N_GX, N_GY, N_GZ, TPD, 3, ATOMS)
    inside = box_side * jax.random.uniform(key, full_shape, jnp.float32)
    component = lax.broadcasted_iota(jnp.int32, full_shape, 4)
    corner = jnp.where(component == 0, lax.broadcasted_iota(jnp.int32, full_shape, 0), jnp.where(component == 1, lax.broadcasted_iota(jnp.int32, full_shape, 1), lax.broadcasted_iota(jnp.int32, full_shape, 2)))
    return corner.astype(jnp.float32) * box_side + inside


def draw_counts(key, part):
    full_shape = (N_GX, N_GY, N_GZ, TPD)
    total_slots = N_GX * N_GY * N_GZ * TPD
    key_size, key_taken, key_spot = jax.random.split(jax.random.fold_in(key, 11), 3)
    sizes = jax.random.randint(key_size, full_shape, ATOMS // 4, ATOMS + 1)
    taken = jax.random.randint(key_taken, full_shape, 0, 5) < 2
    filled = jnp.where(taken, sizes, 0).reshape(total_slots)
    spot = jax.random.randint(key_spot, (), 0, total_slots)
    filled = jnp.where(lax.broadcasted_iota(jnp.int32, (total_slots,), 0) == spot, ATOMS, filled)
    return filled.reshape(full_shape).astype(jnp.int32)


def draw_neighbours(key, part):
    rows_total = N_GX * N_GY * N_GZ * TPD
    near_total = 27 * TPD
    tile_counts = draw_counts(key, part)
    padded = jnp.pad(tile_counts, ((1, 1), (1, 1), (1, 1), (0, 0)))
    blocks = []
    for shift_x in range(3):
        for shift_y in range(3):
            for shift_z in range(3):
                blocks.append(padded[shift_x:shift_x + N_GX, shift_y:shift_y + N_GY, shift_z:shift_z + N_GZ, :])
    near_counts = jnp.stack(blocks, axis=3).reshape(N_GX * N_GY * N_GZ, near_total)
    near_counts = jnp.repeat(near_counts, TPD, axis=0)
    key_perm, key_length = jax.random.split(jax.random.fold_in(key, 23))
    row_keys = jax.random.split(key_perm, rows_total)
    ranks = jax.vmap(lambda row_key: jax.random.permutation(row_key, near_total))(row_keys).astype(jnp.int32)
    own_slot = (13 * TPD + lax.broadcasted_iota(jnp.int32, (rows_total, 1), 0) % TPD).astype(jnp.int32)
    column_all = lax.broadcasted_iota(jnp.int32, (rows_total, near_total), 1)
    eligible = (near_counts > 0) & (column_all != own_slot)
    scores = ranks + eligible.astype(jnp.int32) * near_total
    top_scores, chosen = lax.top_k(scores, NBR - 1)
    chosen = chosen.astype(jnp.int32)
    chosen_ok = top_scores >= near_total
    lengths = jax.random.randint(key_length, (rows_total, 1), max(NBR // 2, 1), NBR + 1)
    column = lax.broadcasted_iota(jnp.int32, (rows_total, NBR - 1), 1) + 1
    chosen = jnp.where(chosen_ok & (column < lengths), chosen, -1)
    listed = jnp.concatenate([own_slot, chosen], axis=1)
    return listed.reshape(N_GX, N_GY, N_GZ, TPD, NBR).astype(jnp.int32)


def steps_of(rng, extent, pieces, low, high):
    level = 1.0
    for axis_at, shards_of in pieces:
        heights = jax.random.uniform(jax.random.fold_in(jax.random.fold_in(rng, 6), axis_at), (shards_of,), jnp.float32, low / len(pieces), high / len(pieces))
        level = level * jnp.repeat(jnp.exp(heights), extent[axis_at] // shards_of).reshape((-1,) + (1,) * (len(extent) - 1 - axis_at))
    return level


def noise(key, shape, width, bound, cuts=(), kind=jnp.bfloat16):
    values = width * jax.random.normal(key, shape, jnp.float32)
    if cuts:
        values = values * steps_of(key, shape, cuts, -0.22, 0.18)
    return jnp.clip(values, -bound, bound).astype(kind)


def setup_inputs(seed: int = 0) -> dict:
    streams_of = jax.random.split(jax.random.key(seed), 8)
    positions = draw_positions(jax.random.fold_in(streams_of[7], 71), 0)
    features = noise(streams_of[1], (N_GX, N_GY, N_GZ, TPD, ATOMS, CH), 1.0, 6.0, ((0, 4), (1, 16), (2, 16)))
    counts = draw_counts(jax.random.fold_in(streams_of[7], 71), 0)
    neighbours = draw_neighbours(jax.random.fold_in(streams_of[7], 71), 0)
    mix_weight = noise(streams_of[4], (2 * RAD * CH, CH), (2 * RAD * CH) ** -0.5, 0.1875)
    readout = noise(streams_of[5], (CH,), 1.0, 4.0, (), jnp.float32)
    radial_rates = jnp.clip(jnp.exp(jax.random.uniform(streams_of[6], (RAD,), jnp.float32, math.log(0.03), math.log(0.6))), 0.03, 0.6)
    return {"positions": positions, "features": features, "counts": counts, "neighbours": neighbours, "mix_weight": mix_weight, "readout": readout, "radial_rates": radial_rates}


def build_basis(own_points, other_points, decay_rates):
    offset = other_points[None, :, :] - jnp.transpose(own_points)[:, :, None]
    square_dist = jnp.sum(offset * offset, axis=1)
    radial = jnp.exp(-decay_rates[None, :, None] * square_dist[:, None, :])
    pair_basis = jnp.concatenate([radial[:, :, None, :], radial[:, :, None, :] * offset[:, None, :, :]], axis=2)
    return offset, radial, pair_basis


def device_terms(own_points, own_valid, own_counts, near_points, near_features, neighbour_rows, mixing, readout, decay_rates):
    tile_count = own_points.shape[0]
    atom_count = own_points.shape[2]
    channel_count = near_features.shape[2]
    slot_count = neighbour_rows.shape[1]
    radial_count = decay_rates.shape[0]
    basis_count = 4 * radial_count
    scaling = (slot_count * atom_count) ** -0.5
    pair_count = tile_count * slot_count
    row_width = (3 + channel_count) * atom_count

    def locate(pair_index):
        tile_index = pair_index // slot_count
        slot_index = pair_index % slot_count
        target = neighbour_rows[tile_index, slot_index]
        is_live = target >= 0
        source_index = jnp.maximum(target, 0)
        return tile_index, source_index, is_live

    def forward_pair(pair_index, summed):
        tile_index, source_index, is_live = locate(pair_index)
        near_tile = jnp.where(is_live, near_features[source_index], jnp.zeros((), jnp.bfloat16))
        offset, radial, pair_basis = build_basis(own_points[tile_index], near_points[source_index], decay_rates)
        flat_basis = pair_basis.reshape(atom_count * basis_count, atom_count).astype(jnp.bfloat16)
        contribution = jnp.dot(flat_basis, near_tile, preferred_element_type=jnp.float32)
        return lax.dynamic_update_index_in_dim(summed, summed[tile_index] + contribution, tile_index, 0)

    summed = lax.fori_loop(0, pair_count, forward_pair, jnp.zeros((tile_count, atom_count * basis_count, channel_count), jnp.float32))
    scaled_sum = summed.reshape(tile_count, atom_count, radial_count, 4, channel_count) * scaling
    scalar_part = scaled_sum[:, :, :, 0, :]
    vector_norm = jnp.sum(scaled_sum[:, :, :, 1:, :] * scaled_sum[:, :, :, 1:, :], axis=3)
    invariant = jnp.concatenate([scalar_part, vector_norm], axis=2).reshape(tile_count * atom_count, 2 * radial_count * channel_count).astype(jnp.bfloat16)
    preact = jnp.dot(invariant, mixing, preferred_element_type=jnp.float32)
    sigmoid_value = jax.nn.sigmoid(preact)
    grad_pre = (own_valid.reshape(-1, 1) * readout[None, :] * sigmoid_value * (1.0 + preact * (1.0 - sigmoid_value))).astype(jnp.bfloat16)
    grad_invariant = lax.dot_general(grad_pre, mixing, (((1,), (1,)), ((), ())), preferred_element_type=jnp.float32)
    grad_invariant = grad_invariant.reshape(tile_count, atom_count, 2, radial_count, channel_count)
    grad_sum = jnp.concatenate([grad_invariant[:, :, 0, :, None, :], 2.0 * scaled_sum[:, :, :, 1:, :] * grad_invariant[:, :, 1, :, None, :]], axis=3) * scaling
    grad_sum = grad_sum.reshape(tile_count, atom_count * basis_count, channel_count).astype(jnp.bfloat16)

    def backward_pair(pair_index, state_pair):
        own_force, ghost_sum = state_pair
        tile_index, source_index, is_live = locate(pair_index)
        near_tile = jnp.where(is_live, near_features[source_index], jnp.zeros((), jnp.bfloat16))
        offset, radial, pair_basis = build_basis(own_points[tile_index], near_points[source_index], decay_rates)
        flat_basis = pair_basis.reshape(atom_count * basis_count, atom_count).astype(jnp.bfloat16)
        seed_rows = grad_sum[tile_index]
        grad_basis = lax.dot_general(seed_rows, near_tile, (((1,), (1,)), ((), ())), preferred_element_type=jnp.float32)
        grad_basis = grad_basis.reshape(atom_count, radial_count, 4, atom_count)
        grad_near = lax.dot_general(flat_basis, seed_rows, (((0,), (0,)), ((), ())), preferred_element_type=jnp.float32)
        inner_term = grad_basis[:, :, 0, :] + jnp.sum(grad_basis[:, :, 1:, :] * offset[:, None, :, :], axis=2)
        pair_force = jnp.sum(radial[:, :, None, :] * (grad_basis[:, :, 1:, :] - 2.0 * decay_rates[None, :, None, None] * offset[:, None, :, :] * inner_term[:, :, None, :]), axis=1)
        own_part = jnp.transpose(jnp.sum(pair_force, axis=2))
        ghost_part = jnp.concatenate([-jnp.sum(pair_force, axis=0).reshape(-1), grad_near.reshape(-1)]) * is_live.astype(jnp.float32)
        own_force = lax.dynamic_update_index_in_dim(own_force, own_force[tile_index] + own_part, tile_index, 0)
        ghost_sum = lax.dynamic_update_index_in_dim(ghost_sum, ghost_sum[source_index] + ghost_part, source_index, 0)
        return own_force, ghost_sum

    start_pair = (jnp.zeros((tile_count, 3, atom_count), jnp.float32), jnp.zeros((27 * tile_count, row_width), jnp.float32))
    return lax.fori_loop(0, pair_count, backward_pair, start_pair)


def reference(positions, features, counts, neighbours, mix_weight, readout, radial_rates):
    device_total = N_GX * N_GY * N_GZ
    row_width = (3 + CH) * ATOMS
    is_valid = lax.broadcasted_iota(jnp.int32, counts.shape + (ATOMS,), 4) < counts[..., None]
    valid_float = is_valid.astype(jnp.float32)
    masked = jnp.where(is_valid[..., None], features, jnp.zeros((), jnp.bfloat16))
    edge_pad = ((1, 1), (1, 1), (1, 1), (0, 0), (0, 0), (0, 0))
    padded_points = jnp.pad(positions, edge_pad)
    padded_features = jnp.pad(masked, edge_pad)
    flat_points = positions.reshape(device_total, TPD, 3, ATOMS)
    flat_valid = valid_float.reshape(device_total, TPD, ATOMS)
    flat_counts = counts.reshape(device_total, TPD)
    flat_rows = neighbours.reshape(device_total, TPD, NBR)
    zero_index = jnp.zeros((), jnp.int32)

    def device_step(totals, device_flat):
        coord_x = (device_flat // (N_GY * N_GZ)).astype(jnp.int32)
        coord_y = ((device_flat // N_GZ) % N_GY).astype(jnp.int32)
        coord_z = (device_flat % N_GZ).astype(jnp.int32)
        near_points = lax.dynamic_slice(padded_points, (coord_x, coord_y, coord_z, zero_index, zero_index, zero_index), (3, 3, 3, TPD, 3, ATOMS)).reshape(27 * TPD, 3, ATOMS)
        near_features = lax.dynamic_slice(padded_features, (coord_x, coord_y, coord_z, zero_index, zero_index, zero_index), (3, 3, 3, TPD, ATOMS, CH)).reshape(27 * TPD, ATOMS, CH)
        own_force, ghost_sum = device_terms(flat_points[device_flat], flat_valid[device_flat], flat_counts[device_flat], near_points, near_features, flat_rows[device_flat], mix_weight, readout, radial_rates)
        start = (coord_x, coord_y, coord_z, zero_index, zero_index)
        region = lax.dynamic_slice(totals, start, (3, 3, 3, TPD, row_width)) + ghost_sum.reshape(3, 3, 3, TPD, row_width)
        return lax.dynamic_update_slice(totals, region, start), own_force

    totals = jnp.zeros((N_GX + 2, N_GY + 2, N_GZ + 2, TPD, row_width), jnp.float32)
    totals, own_forces = lax.scan(device_step, totals, jnp.arange(device_total, dtype=jnp.int32))
    interior = totals[1:-1, 1:-1, 1:-1]
    forces = own_forces.reshape(N_GX, N_GY, N_GZ, TPD, 3, ATOMS) + interior[..., :3 * ATOMS].reshape(N_GX, N_GY, N_GZ, TPD, 3, ATOMS)
    feature_grads = interior[..., 3 * ATOMS:].reshape(N_GX, N_GY, N_GZ, TPD, ATOMS, CH) * valid_float[..., None]
    return forces, feature_grads
```

```python
import functools

import jax
import jax.numpy as jnp
from jax import lax
from jax.experimental import pallas as pl
from jax.experimental.pallas import tpu as pltpu
from jax.sharding import PartitionSpec as P

A = 128
C = 128
R = 4
S = 8
T = 2
NEAR = 27 * T
ROWS = 136
SCALING = (S * A) ** -0.5
CHUNK = 32


def extended(block, sides, width):
    for axis, dim in sides:
        count = lax.axis_size(axis)
        forward = [(i, i + 1) for i in range(count - 1)]
        backward = [(target, source) for source, target in forward]
        low = lax.ppermute(
            lax.slice_in_dim(block, block.shape[dim] - width, None, axis=dim), axis, forward
        )
        high = lax.ppermute(lax.slice_in_dim(block, 0, width, axis=dim), axis, backward)
        block = jnp.concatenate([low, block, high], axis=dim)
    return block


def from_behind(block, axis, distance):
    devices = range(lax.axis_size(axis))
    route = [(i - distance, i) for i in devices if i - distance in devices]
    return lax.ppermute(block, axis, route)


def fold_plane(buffer, axis_dim, sender):
    lower_plane = lax.slice_in_dim(buffer, 0, 1, axis=axis_dim)
    middle_plane = lax.slice_in_dim(buffer, 1, 2, axis=axis_dim)
    upper_plane = lax.slice_in_dim(buffer, 2, 3, axis=axis_dim)
    result = middle_plane
    for toward in (1, -1):
        result = result + sender(upper_plane if toward == 1 else lower_plane, toward)
    return result


def pair_geometry(near, own, base, size):
    offset = [near[m : m + 1, :] - own[m, pl.ds(base, size), :] for m in range(3)]
    square = offset[0] * offset[0] + offset[1] * offset[1] + offset[2] * offset[2]
    return offset, square


def tile_terms(
    t, nbr, counts, rates, pos, near_pos, near_feat, mix, readout,
    own, basis, stack, sums, inv, grad, gbuf, own_acc, contrib, contrib_force, own_force,
):
    for m in range(3):
        own[m] = jnp.transpose(jnp.broadcast_to(pos[t, m : m + 1, :], (A, A)))
        own_acc[m] = jnp.zeros((A, A), jnp.float32)

    def build(s, carry):
        n = nbr[t * S + s]
        source = jnp.maximum(n, 0)
        near = near_pos[source]
        lanes = pl.ds(pl.multiple_of(s * A, A), A)
        tile = near_feat[source]
        stack[lanes, :] = jnp.where(n >= 0, tile, jnp.zeros_like(tile))
        for base in range(0, A, CHUNK):
            offset, square = pair_geometry(near, own, base, CHUNK)
            for r in range(R):
                g = jnp.exp(-rates[r] * square)
                for m in range(4):
                    value = g if m == 0 else g * offset[m - 1]
                    row = (r * 4 + m) * A + base
                    basis[row : row + CHUNK, lanes] = value.astype(jnp.bfloat16)
        return carry

    lax.fori_loop(0, S, build, 0)

    def forward(k, carry):
        rows = pl.ds(pl.multiple_of(k * 4 * A, 4 * A), 4 * A)
        sums[rows, :] = jnp.dot(basis[rows, :], stack[...], preferred_element_type=jnp.float32) * SCALING
        return carry

    lax.fori_loop(0, R, forward, 0)

    for r in range(R):
        base = r * 4 * A
        inv[:, r * C : (r + 1) * C] = sums[base : base + A, :].astype(jnp.bfloat16)
        total = jnp.zeros((A, C), jnp.float32)
        for m in range(1, 4):
            part = sums[base + m * A : base + (m + 1) * A, :]
            total = total + part * part
        inv[:, (R + r) * C : (R + r + 1) * C] = total.astype(jnp.bfloat16)
    preact = jnp.dot(inv[...], mix[...], preferred_element_type=jnp.float32)
    sigmoid = 1.0 / (1.0 + jnp.exp(-preact))
    valid = lax.broadcasted_iota(jnp.int32, (A, C), 0) < counts[t]
    grad_pre = readout[...] * sigmoid * (1.0 + preact * (1.0 - sigmoid))
    grad_pre = jnp.where(valid, grad_pre, 0.0).astype(jnp.bfloat16)
    for r in range(R):
        base = r * 4 * A
        for half in range(2):
            k = half * R + r
            gi = lax.dot_general(
                grad_pre, mix[k * C : (k + 1) * C, :], (((1,), (1,)), ((), ())),
                preferred_element_type=jnp.float32,
            )
            if half == 0:
                grad[base : base + A, :] = (gi * SCALING).astype(jnp.bfloat16)
            else:
                for m in range(1, 4):
                    rows = slice(base + m * A, base + (m + 1) * A)
                    grad[rows, :] = (2.0 * sums[rows, :] * gi * SCALING).astype(jnp.bfloat16)

    def backward(p, carry):
        wide = pl.ds(pl.multiple_of(p * 2 * A, 2 * A), 2 * A)
        near_grad = lax.dot_general(
            basis[:, wide], grad[...], (((0,), (0,)), ((), ())), preferred_element_type=jnp.float32
        )
        pair = t * S + p * 2
        contrib[pair] = near_grad[:A]
        contrib[pair + 1] = near_grad[A:]
        gbuf[...] = lax.dot_general(
            grad[...], stack[wide, :], (((1,), (1,)), ((), ())), preferred_element_type=jnp.float32
        )
        for u in range(2):
            near = near_pos[jnp.maximum(nbr[pair + u], 0)]
            cols = slice(u * A, (u + 1) * A)
            column = [jnp.zeros((8, A), jnp.float32) for _ in range(3)]
            for base in range(0, A, CHUNK):
                offset, square = pair_geometry(near, own, base, CHUNK)
                force = [None] * 3
                pull = None
                for r in range(R):
                    g = jnp.exp(-rates[r] * square)
                    gb = [gbuf[(r * 4 + m) * A + base : (r * 4 + m) * A + base + CHUNK, cols] for m in range(4)]
                    inner = gb[0] + gb[1] * offset[0] + gb[2] * offset[1] + gb[3] * offset[2]
                    term = (2.0 * rates[r]) * g * inner
                    pull = term if pull is None else pull + term
                    for m in range(3):
                        part = g * gb[m + 1]
                        force[m] = part if force[m] is None else force[m] + part
                for m in range(3):
                    force[m] = force[m] - offset[m] * pull
                    own_acc[m, base : base + CHUNK, :] += force[m]
                    for k in range(0, CHUNK, 8):
                        column[m] = column[m] + force[m][k : k + 8]
            for m in range(3):
                contrib_force[pair + u, m : m + 1, :] = -jnp.sum(column[m], axis=0, keepdims=True)
        return carry

    lax.fori_loop(0, S // 2, backward, 0)
    for m in range(3):
        own_force[t, m : m + 1, :] = jnp.sum(jnp.transpose(own_acc[m]), axis=0, keepdims=True)


def compute_kernel(
    nbr, inverse, counts, rates, pos, near_pos, near_feat, mix, readout,
    own_force, ghost,
    own, basis, stack, sums, inv, grad, gbuf, own_acc, contrib, contrib_force,
):
    def one_tile(t, carry):
        tile_terms(
            t, nbr, counts, rates, pos, near_pos, near_feat, mix, readout,
            own, basis, stack, sums, inv, grad, gbuf, own_acc, contrib, contrib_force, own_force,
        )
        return carry

    lax.fori_loop(0, T, one_tile, 0)

    def gather(n, carry):
        block = jnp.zeros((A, C), jnp.float32)
        force = jnp.zeros((8, A), jnp.float32)
        for t in range(T):
            s = inverse[t * NEAR + n]
            pair = t * S + jnp.maximum(s, 0)
            block = block + jnp.where(s >= 0, contrib[pair], 0.0)
            force = force + jnp.where(s >= 0, contrib_force[pair], 0.0)
        ghost[n, 0:A, :] = block
        ghost[n, A:ROWS, :] = force
        return carry

    lax.fori_loop(0, NEAR, gather, 0)


def compute(nbr, counts, rates, pos, near_pos, near_feat, mix, readout):
    flat = nbr.reshape(T * S)
    where = jnp.where(
        nbr[:, :, None] == lax.broadcasted_iota(jnp.int32, (T, S, NEAR), 2),
        lax.broadcasted_iota(jnp.int32, (T, S, NEAR), 1),
        -1,
    )
    inverse = jnp.max(where, axis=1).reshape(T * NEAR)
    smem = pl.BlockSpec(memory_space=pltpu.SMEM)
    vmem = pl.BlockSpec(memory_space=pltpu.VMEM)
    return pl.pallas_call(
        compute_kernel,
        out_shape=(
            jax.ShapeDtypeStruct((T, 3, A), jnp.float32),
            jax.ShapeDtypeStruct((NEAR, ROWS, C), jnp.float32),
        ),
        in_specs=[smem] * 4 + [vmem] * 5,
        out_specs=(vmem, vmem),
        scratch_shapes=[
            pltpu.VMEM((3, A, A), jnp.float32),
            pltpu.VMEM((4 * R * A, S * A), jnp.bfloat16),
            pltpu.VMEM((S * A, C), jnp.bfloat16),
            pltpu.VMEM((4 * R * A, C), jnp.float32),
            pltpu.VMEM((A, 2 * R * C), jnp.bfloat16),
            pltpu.VMEM((4 * R * A, C), jnp.bfloat16),
            pltpu.VMEM((4 * R * A, 2 * A), jnp.float32),
            pltpu.VMEM((3, A, A), jnp.float32),
            pltpu.VMEM((T * S, A, C), jnp.float32),
            pltpu.VMEM((T * S, 8, A), jnp.float32),
        ],
        compiler_params=pltpu.CompilerParams(vmem_limit_bytes=48 * 1024 * 1024),
    )(flat, inverse, counts, rates, pos, near_pos, near_feat, mix, readout)


def body(positions, features, counts, neighbours, mix_weight, readout, radial_rates):
    own_counts = counts.reshape(T)
    is_valid = lax.broadcasted_iota(jnp.int32, (T, A), 1) < own_counts[:, None]
    masked = jnp.where(is_valid.reshape(1, 1, 1, T, A, 1), features, jnp.zeros((), jnp.bfloat16))
    near_points = extended(positions, (("gx", 0), ("gy", 1), ("gz", 2)), 1)
    near_features = extended(masked, (("gx", 0), ("gy", 1), ("gz", 2)), 1)
    own_force, ghost = compute(
        neighbours.reshape(T, S),
        own_counts,
        radial_rates,
        positions.reshape(T, 3, A),
        near_points.reshape(NEAR, 3, A),
        near_features.reshape(NEAR, A, C),
        mix_weight,
        readout.reshape(1, C),
    )
    buffer = ghost.reshape(3, 3, 3, T, ROWS, C)
    buffer = fold_plane(buffer, 2, lambda values, toward: from_behind(values, "gz", toward))
    buffer = fold_plane(buffer, 1, lambda values, toward: from_behind(values, "gy", toward))
    buffer = fold_plane(buffer, 0, lambda values, toward: from_behind(values, "gx", toward))
    center = buffer.reshape(T, ROWS, C)
    forces = own_force + center[:, A : A + 3, :]
    feature_grads = jnp.where(is_valid[:, :, None], center[:, :A, :], 0.0)
    return (
        forces.reshape(1, 1, 1, T, 3, A),
        feature_grads.reshape(1, 1, 1, T, A, C),
    )


def solution(mesh):
    cell = ("gx", "gy", "gz")
    in_specs = (
        P(*cell, None, None, None),
        P(*cell, None, None, None),
        P(*cell, None),
        P(*cell, None, None),
        P(),
        P(),
        P(),
    )
    out_specs = (P(*cell, None, None, None), P(*cell, None, None, None))
    return jax.shard_map(body, mesh=mesh, in_specs=in_specs, out_specs=out_specs, check_vma=False)
```

```python
import functools

import jax
import jax.numpy as jnp
from jax import lax
from jax.experimental import pallas as pl
from jax.experimental.pallas import tpu as pltpu
from jax.sharding import PartitionSpec as P

A = 128
C = 128
R = 4
S = 8
T = 2
NEAR = 27 * T
ROWS = 136
SCALING = (S * A) ** -0.5
CHUNK = 32


def pair_geometry(near, own, base, size):
    offset = [near[m : m + 1, :] - own[m, pl.ds(base, size), :] for m in range(3)]
    square = offset[0] * offset[0] + offset[1] * offset[1] + offset[2] * offset[2]
    return offset, square


def tile_terms(
    t, nbr, counts, rates, pos, near_pos, near_feat, mix, readout,
    own, basis, stack, sums, inv, grad, gbuf, own_acc, contrib, contrib_force, own_force,
):
    for m in range(3):
        own[m] = jnp.transpose(jnp.broadcast_to(pos[t, m : m + 1, :], (A, A)))
        own_acc[m] = jnp.zeros((A, A), jnp.float32)

    def build(s, carry):
        n = nbr[t * S + s]
        source = jnp.maximum(n, 0)
        near = near_pos[source]
        lanes = pl.ds(pl.multiple_of(s * A, A), A)
        tile = near_feat[source]
        stack[lanes, :] = jnp.where(n >= 0, tile, jnp.zeros_like(tile))
        for base in range(0, A, CHUNK):
            offset, square = pair_geometry(near, own, base, CHUNK)
            for r in range(R):
                g = jnp.exp(-rates[r] * square)
                for m in range(4):
                    value = g if m == 0 else g * offset[m - 1]
                    row = (r * 4 + m) * A + base
                    basis[row : row + CHUNK, lanes] = value.astype(jnp.bfloat16)
        return carry

    lax.fori_loop(0, S, build, 0)

    def forward(k, carry):
        rows = pl.ds(pl.multiple_of(k * 4 * A, 4 * A), 4 * A)
        sums[rows, :] = jnp.dot(basis[rows, :], stack[...], preferred_element_type=jnp.float32) * SCALING
        return carry

    lax.fori_loop(0, R, forward, 0)

    for r in range(R):
        base = r * 4 * A
        inv[:, r * C : (r + 1) * C] = sums[base : base + A, :].astype(jnp.bfloat16)
        total = jnp.zeros((A, C), jnp.float32)
        for m in range(1, 4):
            part = sums[base + m * A : base + (m + 1) * A, :]
            total = total + part * part
        inv[:, (R + r) * C : (R + r + 1) * C] = total.astype(jnp.bfloat16)
    preact = jnp.dot(inv[...], mix[...], preferred_element_type=jnp.float32)
    sigmoid = 1.0 / (1.0 + jnp.exp(-preact))
    valid = lax.broadcasted_iota(jnp.int32, (A, C), 0) < counts[t]
    grad_pre = readout[...] * sigmoid * (1.0 + preact * (1.0 - sigmoid))
    grad_pre = jnp.where(valid, grad_pre, 0.0).astype(jnp.bfloat16)
    for r in range(R):
        base = r * 4 * A
        for half in range(2):
            k = half * R + r
            gi = lax.dot_general(
                grad_pre, mix[k * C : (k + 1) * C, :], (((1,), (1,)), ((), ())),
                preferred_element_type=jnp.float32,
            )
            if half == 0:
                grad[base : base + A, :] = (gi * SCALING).astype(jnp.bfloat16)
            else:
                for m in range(1, 4):
                    rows = slice(base + m * A, base + (m + 1) * A)
                    grad[rows, :] = (2.0 * sums[rows, :] * gi * SCALING).astype(jnp.bfloat16)

    def backward(p, carry):
        wide = pl.ds(pl.multiple_of(p * 2 * A, 2 * A), 2 * A)
        near_grad = lax.dot_general(
            basis[:, wide], grad[...], (((0,), (0,)), ((), ())), preferred_element_type=jnp.float32
        )
        pair = t * S + p * 2
        contrib[pair] = near_grad[:A]
        contrib[pair + 1] = near_grad[A:]
        gbuf[...] = lax.dot_general(
            grad[...], stack[wide, :], (((1,), (1,)), ((), ())), preferred_element_type=jnp.float32
        )
        for u in range(2):
            near = near_pos[jnp.maximum(nbr[pair + u], 0)]
            cols = slice(u * A, (u + 1) * A)
            column = [jnp.zeros((8, A), jnp.float32) for _ in range(3)]
            for base in range(0, A, CHUNK):
                offset, square = pair_geometry(near, own, base, CHUNK)
                force = [None] * 3
                pull = None
                for r in range(R):
                    g = jnp.exp(-rates[r] * square)
                    gb = [gbuf[(r * 4 + m) * A + base : (r * 4 + m) * A + base + CHUNK, cols] for m in range(4)]
                    inner = gb[0] + gb[1] * offset[0] + gb[2] * offset[1] + gb[3] * offset[2]
                    term = (2.0 * rates[r]) * g * inner
                    pull = term if pull is None else pull + term
                    for m in range(3):
                        part = g * gb[m + 1]
                        force[m] = part if force[m] is None else force[m] + part
                for m in range(3):
                    force[m] = force[m] - offset[m] * pull
                    own_acc[m, base : base + CHUNK, :] += force[m]
                    for k in range(0, CHUNK, 8):
                        column[m] = column[m] + force[m][k : k + 8]
            contrib_force[pair + u] = jnp.zeros((8, A), jnp.float32)
            for m in range(3):
                contrib_force[pair + u, m : m + 1, :] = -jnp.sum(column[m], axis=0, keepdims=True)
        return carry

    lax.fori_loop(0, S // 2, backward, 0)
    for m in range(3):
        own_force[t, m : m + 1, :] = jnp.sum(jnp.transpose(own_acc[m]), axis=0, keepdims=True)


MESH = pl.DeviceIdType.MESH
PLANE = [(dy, dz) for dy in (-1, 0, 1) for dz in (-1, 0, 1) if (dy, dz) != (0, 0)]


def cell_of(dy, dz):
    return (dy + 1) * 3 + dz + 1


def step_kernel(
    nbr, inverse, counts, rates, pos, feat, mix, readout,
    forces, feature_grads,
    near_feat, near_pos, own, basis, stack, sums, inv, grad, gbuf, own_acc, own_force, contrib, contrib_force,
    plane_out, plane_in, far_out, far_in, pair_out, pair_in, far_sum, far_got, total,
    feat_send, feat_recv, pos_send, pos_recv, grad_send, grad_recv,
):
    x, y, z = lax.axis_index("gx"), lax.axis_index("gy"), lax.axis_index("gz")
    ny, nz = lax.axis_size("gy"), lax.axis_size("gz")
    toward = 1 - 2 * lax.rem(x, 2)
    partner = (x + toward, y, z)
    across = (x - toward, y, z)
    has_far = (x - toward >= 0) & (x - toward < lax.axis_size("gx"))
    pair_base = (toward + 1) * 9
    far_base = (1 - toward) * 9
    around = []
    for dy, dz in PLANE:
        exists = (y + dy >= 0) & (y + dy < ny) & (z + dz >= 0) & (z + dz < nz)
        around.append((dy, dz, (x, y + dy, z + dz), exists))

    zero_feat = jnp.zeros((T, A, C), jnp.bfloat16)
    zero_pos = jnp.zeros((T, 3, A), jnp.float32)

    def clear(c, carry):
        near_feat[pl.ds(c * T, T)] = zero_feat
        near_pos[pl.ds(c * T, T)] = zero_pos
        return carry

    lax.fori_loop(0, 27, clear, 0)

    barrier = pltpu.get_barrier_semaphore()

    @pl.when(has_far)
    def _():
        pl.semaphore_signal(barrier, inc=1, device_id=across, device_id_type=MESH)

    for dy, dz, there, exists in around:
        @pl.when(exists)
        def _():
            pl.semaphore_signal(barrier, inc=1, device_id=there, device_id_type=MESH)

    pl.semaphore_signal(barrier, inc=1, device_id=partner, device_id_type=MESH)
    rows_near = 3 - jnp.where(y == 0, 1, 0) - jnp.where(y == ny - 1, 1, 0)
    columns_near = 3 - jnp.where(z == 0, 1, 0) - jnp.where(z == nz - 1, 1, 0)
    pl.semaphore_wait(barrier, rows_near * columns_near + jnp.where(has_far, 1, 0))

    def send_cell(feat_from, pos_from, cell, k, there):
        rows = pl.ds(cell * T, T)
        return (
            pltpu.make_async_remote_copy(
                feat_from, near_feat.at[rows], feat_send.at[k], feat_recv.at[k], device_id=there, device_id_type=MESH
            ),
            pltpu.make_async_remote_copy(
                pos_from, near_pos.at[rows], pos_send.at[k], pos_recv.at[k], device_id=there, device_id_type=MESH
            ),
        )

    def start(copies):
        for copy in copies:
            copy.start()

    def arrive(copies):
        for copy in copies:
            copy.wait_recv()

    def leave(copies):
        for copy in copies:
            copy.wait_send()

    own_sends = []
    far_sends = []
    pair_sends = []
    far_rows = pl.ds((far_base + 4) * T, T)
    far_copy = send_cell(feat, pos, (pair_base + 4), 25, across)
    for k, (dy, dz, there, exists) in enumerate(around):
        own_sends.append(send_cell(feat, pos, 9 + cell_of(-dy, -dz), k, there))
        far_sends.append(
            send_cell(near_feat.at[far_rows], near_pos.at[far_rows], far_base + cell_of(-dy, -dz), 8 + k, there)
        )
        rows = pl.ds((9 + cell_of(dy, dz)) * T, T)
        pair_sends.append(
            send_cell(near_feat.at[rows], near_pos.at[rows], far_base + cell_of(dy, dz), 16 + k, partner)
        )
    centre_send = send_cell(feat, pos, far_base + 4, 24, partner)

    @pl.when(has_far)
    def _():
        start(far_copy)

    for k in range(8):
        @pl.when(around[k][3])
        def _():
            start(own_sends[k])

    start(centre_send)
    near_feat[13 * T : 14 * T] = feat[...]
    near_pos[13 * T : 14 * T] = pos[...]
    for k in range(8):
        @pl.when(around[k][3])
        def _():
            arrive(own_sends[7 - k])
            start(pair_sends[k])

    @pl.when(has_far)
    def _():
        arrive(far_copy)
        for k in range(8):
            @pl.when(around[k][3])
            def _():
                start(far_sends[k])

    for k in range(8):
        @pl.when(around[k][3])
        def _():
            arrive(pair_sends[k])

    arrive(centre_send)

    @pl.when(has_far)
    def _():
        for k in range(8):
            @pl.when(around[k][3])
            def _():
                arrive(far_sends[7 - k])

    def one_tile(t, carry):
        tile_terms(
            t, nbr, counts, rates, pos, near_pos, near_feat, mix, readout,
            own, basis, stack, sums, inv, grad, gbuf, own_acc, contrib, contrib_force, own_force,
        )
        return carry

    lax.fori_loop(0, T, one_tile, 0)

    def collect(cell, u):
        block = jnp.zeros((A, C), jnp.float32)
        force = jnp.zeros((8, A), jnp.float32)
        for t in range(T):
            s = inverse[t * NEAR + cell * T + u]
            pair = t * S + jnp.maximum(s, 0)
            block = block + jnp.where(s >= 0, contrib[pair], 0.0)
            force = force + jnp.where(s >= 0, contrib_force[pair], 0.0)
        return block, force

    def fill(ref, cell):
        def one(u, carry):
            block, force = collect(cell, u)
            ref[u, 0:A, :] = block
            ref[u, A:ROWS, :] = force
            return carry

        lax.fori_loop(0, T, one, 0)

    def send_grad(from_ref, to_ref, k, there):
        return pltpu.make_async_remote_copy(
            from_ref, to_ref, grad_send.at[k], grad_recv.at[k], device_id=there, device_id_type=MESH
        )

    far_grads = [send_grad(far_out.at[k], far_in.at[k], k, around[k][2]) for k in range(8)]
    own_grads = [send_grad(plane_out.at[k], plane_in.at[k], 8 + k, around[k][2]) for k in range(8)]
    pair_grads = send_grad(pair_out, pair_in, 16, partner)
    far_grad = send_grad(far_sum, far_got, 17, across)

    @pl.when(has_far)
    def _():
        for k, (dy, dz, there, exists) in enumerate(around):
            @pl.when(exists)
            def _():
                fill(far_out.at[k], far_base + cell_of(dy, dz))
                far_grads[k].start()
        fill(far_sum, far_base + 4)

    def pair_cell(c, carry):
        fill(pair_out.at[c], pair_base + c)
        return carry

    lax.fori_loop(0, 9, pair_cell, 0)
    pair_grads.start()

    @pl.when(has_far)
    def _():
        for k in range(8):
            @pl.when(around[k][3])
            def _():
                far_grads[7 - k].wait_recv()
                far_sum[...] += far_in[7 - k]
        far_grad.start()

    fill(total, 13)
    pair_grads.wait_recv()
    for k, (dy, dz, there, exists) in enumerate(around):
        @pl.when(exists)
        def _():
            fill(plane_out.at[k], 9 + cell_of(dy, dz))
            plane_out[k] += pair_in[cell_of(dy, dz)]
            own_grads[k].start()

    total[...] += pair_in[4]
    for k in range(8):
        @pl.when(around[k][3])
        def _():
            own_grads[7 - k].wait_recv()
            total[...] += plane_in[7 - k]

    @pl.when(has_far)
    def _():
        far_grad.wait_recv()
        total[...] += far_got[...]

    for t in range(T):
        valid = lax.broadcasted_iota(jnp.int32, (A, C), 0) < counts[t]
        feature_grads[t] = jnp.where(valid, total[t, 0:A, :], 0.0)
        forces[t] = own_force[t] + total[t, A : A + 3, :]

    @pl.when(has_far)
    def _():
        leave(far_copy)
        far_grad.wait_send()
        for k in range(8):
            @pl.when(around[k][3])
            def _():
                leave(far_sends[k])
                far_grads[k].wait_send()

    for k in range(8):
        @pl.when(around[k][3])
        def _():
            leave(own_sends[k])
            leave(pair_sends[k])
            own_grads[k].wait_send()

    leave(centre_send)
    pair_grads.wait_send()


def body(positions, features, counts, neighbours, mix_weight, readout, radial_rates):
    own_counts = counts.reshape(T)
    is_valid = lax.broadcasted_iota(jnp.int32, (T, A, C), 1) < own_counts[:, None, None]
    masked = jnp.where(is_valid, features.reshape(T, A, C), jnp.zeros((), jnp.bfloat16))
    nbr = neighbours.reshape(T, S)
    where = jnp.where(
        nbr[:, :, None] == lax.broadcasted_iota(jnp.int32, (T, S, NEAR), 2),
        lax.broadcasted_iota(jnp.int32, (T, S, NEAR), 1),
        -1,
    )
    inverse = jnp.max(where, axis=1).reshape(T * NEAR)
    smem = pl.BlockSpec(memory_space=pltpu.SMEM)
    vmem = pl.BlockSpec(memory_space=pltpu.VMEM)
    cell = (T, ROWS, C)
    forces, feature_grads = pl.pallas_call(
        step_kernel,
        out_shape=(
            jax.ShapeDtypeStruct((T, 3, A), jnp.float32),
            jax.ShapeDtypeStruct((T, A, C), jnp.float32),
        ),
        in_specs=[smem] * 4 + [vmem] * 4,
        out_specs=(vmem, vmem),
        scratch_shapes=[
            pltpu.VMEM((NEAR, A, C), jnp.bfloat16),
            pltpu.VMEM((NEAR, 3, A), jnp.float32),
            pltpu.VMEM((3, A, A), jnp.float32),
            pltpu.VMEM((4 * R * A, S * A), jnp.bfloat16),
            pltpu.VMEM((S * A, C), jnp.bfloat16),
            pltpu.VMEM((4 * R * A, C), jnp.float32),
            pltpu.VMEM((A, 2 * R * C), jnp.bfloat16),
            pltpu.VMEM((4 * R * A, C), jnp.bfloat16),
            pltpu.VMEM((4 * R * A, 2 * A), jnp.float32),
            pltpu.VMEM((3, A, A), jnp.float32),
            pltpu.VMEM((T, 3, A), jnp.float32),
            pltpu.VMEM((T * S, A, C), jnp.float32),
            pltpu.VMEM((T * S, 8, A), jnp.float32),
            pltpu.VMEM((8, *cell), jnp.float32),
            pltpu.VMEM((8, *cell), jnp.float32),
            pltpu.VMEM((8, *cell), jnp.float32),
            pltpu.VMEM((8, *cell), jnp.float32),
            pltpu.VMEM((9, *cell), jnp.float32),
            pltpu.VMEM((9, *cell), jnp.float32),
            pltpu.VMEM(cell, jnp.float32),
            pltpu.VMEM(cell, jnp.float32),
            pltpu.VMEM(cell, jnp.float32),
            pltpu.SemaphoreType.DMA((26,)),
            pltpu.SemaphoreType.DMA((26,)),
            pltpu.SemaphoreType.DMA((26,)),
            pltpu.SemaphoreType.DMA((26,)),
            pltpu.SemaphoreType.DMA((18,)),
            pltpu.SemaphoreType.DMA((18,)),
        ],
        compiler_params=pltpu.CompilerParams(
            collective_id=0, has_side_effects=True, vmem_limit_bytes=56 * 1024 * 1024
        ),
    )(nbr.reshape(T * S), inverse, own_counts, radial_rates, positions.reshape(T, 3, A), masked, mix_weight, readout.reshape(1, C))
    return (
        forces.reshape(1, 1, 1, T, 3, A),
        feature_grads.reshape(1, 1, 1, T, A, C),
    )


def solution(mesh):
    cell = ("gx", "gy", "gz")
    in_specs = (
        P(*cell, None, None, None),
        P(*cell, None, None, None),
        P(*cell, None),
        P(*cell, None, None),
        P(),
        P(),
        P(),
    )
    out_specs = (P(*cell, None, None, None), P(*cell, None, None, None))
    return jax.shard_map(body, mesh=mesh, in_specs=in_specs, out_specs=out_specs, check_vma=False)
```

```python
import functools

import jax
import jax.numpy as jnp
from jax import lax
from jax.experimental import pallas as pl
from jax.experimental.pallas import tpu as pltpu
from jax.sharding import PartitionSpec as P

A = 128
C = 128
R = 4
S = 8
T = 2
NEAR = 27 * T
ROWS = 136
SCALING = (S * A) ** -0.5
CHUNK = 32


def pair_geometry(near, own, t, base, size):
    offset = [near[m : m + 1, :] - own[t, m, pl.ds(base, size), :] for m in range(3)]
    square = offset[0] * offset[0] + offset[1] * offset[1] + offset[2] * offset[2]
    return offset, square


def tile_gradients(
    t, nbr, counts, rates, pos, near_pos, near_feat, mix, readout, own, basis, stack, sums, inv, grad, contrib
):
    for m in range(3):
        own[t, m] = jnp.transpose(jnp.broadcast_to(pos[t, m : m + 1, :], (A, A)))

    def build(s, carry):
        n = nbr[t * S + s]
        source = jnp.maximum(n, 0)
        near = near_pos[source]
        lanes = pl.ds(pl.multiple_of(s * A, A), A)
        tile = near_feat[source]
        stack[t, lanes, :] = jnp.where(n >= 0, tile, jnp.zeros_like(tile))
        for base in range(0, A, CHUNK):
            offset, square = pair_geometry(near, own, t, base, CHUNK)
            for r in range(R):
                g = jnp.exp(-rates[r] * square)
                for m in range(4):
                    value = g if m == 0 else g * offset[m - 1]
                    row = (r * 4 + m) * A + base
                    basis[t, row : row + CHUNK, lanes] = value.astype(jnp.bfloat16)
        return carry

    lax.fori_loop(0, S, build, 0)

    def forward(k, carry):
        rows = pl.ds(pl.multiple_of(k * 4 * A, 4 * A), 4 * A)
        sums[rows, :] = jnp.dot(basis[t, rows, :], stack[t], preferred_element_type=jnp.float32) * SCALING
        return carry

    lax.fori_loop(0, R, forward, 0)

    for r in range(R):
        base = r * 4 * A
        inv[:, r * C : (r + 1) * C] = sums[base : base + A, :].astype(jnp.bfloat16)
        total = jnp.zeros((A, C), jnp.float32)
        for m in range(1, 4):
            part = sums[base + m * A : base + (m + 1) * A, :]
            total = total + part * part
        inv[:, (R + r) * C : (R + r + 1) * C] = total.astype(jnp.bfloat16)
    preact = jnp.dot(inv[...], mix[...], preferred_element_type=jnp.float32)
    sigmoid = 1.0 / (1.0 + jnp.exp(-preact))
    valid = lax.broadcasted_iota(jnp.int32, (A, C), 0) < counts[t]
    grad_pre = readout[...] * sigmoid * (1.0 + preact * (1.0 - sigmoid))
    grad_pre = jnp.where(valid, grad_pre, 0.0).astype(jnp.bfloat16)
    for r in range(R):
        base = r * 4 * A
        for half in range(2):
            k = half * R + r
            gi = lax.dot_general(
                grad_pre, mix[k * C : (k + 1) * C, :], (((1,), (1,)), ((), ())),
                preferred_element_type=jnp.float32,
            )
            if half == 0:
                grad[t, base : base + A, :] = (gi * SCALING).astype(jnp.bfloat16)
            else:
                for m in range(1, 4):
                    rows = slice(base + m * A, base + (m + 1) * A)
                    grad[t, rows, :] = (2.0 * sums[rows, :] * gi * SCALING).astype(jnp.bfloat16)

    def spread(p, carry):
        wide = pl.ds(pl.multiple_of(p * 2 * A, 2 * A), 2 * A)
        near_grad = lax.dot_general(
            basis[t, :, wide], grad[t], (((0,), (0,)), ((), ())), preferred_element_type=jnp.float32
        )
        pair = t * S + p * 2
        contrib[pair] = near_grad[:A]
        contrib[pair + 1] = near_grad[A:]
        return carry

    lax.fori_loop(0, S // 2, spread, 0)


def tile_forces(t, nbr, rates, near_pos, own, stack, grad, gbuf, own_acc, contrib_force, own_force):
    for m in range(3):
        own_acc[m] = jnp.zeros((A, A), jnp.float32)

    def backward(p, carry):
        wide = pl.ds(pl.multiple_of(p * 2 * A, 2 * A), 2 * A)
        pair = t * S + p * 2
        gbuf[...] = lax.dot_general(
            grad[t], stack[t, wide, :], (((1,), (1,)), ((), ())), preferred_element_type=jnp.float32
        )
        for u in range(2):
            near = near_pos[jnp.maximum(nbr[pair + u], 0)]
            cols = slice(u * A, (u + 1) * A)
            column = [jnp.zeros((8, A), jnp.float32) for _ in range(3)]
            for base in range(0, A, CHUNK):
                offset, square = pair_geometry(near, own, t, base, CHUNK)
                force = [None] * 3
                pull = None
                for r in range(R):
                    g = jnp.exp(-rates[r] * square)
                    gb = [gbuf[(r * 4 + m) * A + base : (r * 4 + m) * A + base + CHUNK, cols] for m in range(4)]
                    inner = gb[0] + gb[1] * offset[0] + gb[2] * offset[1] + gb[3] * offset[2]
                    term = (2.0 * rates[r]) * g * inner
                    pull = term if pull is None else pull + term
                    for m in range(3):
                        part = g * gb[m + 1]
                        force[m] = part if force[m] is None else force[m] + part
                for m in range(3):
                    force[m] = force[m] - offset[m] * pull
                    own_acc[m, base : base + CHUNK, :] += force[m]
                    for k in range(0, CHUNK, 8):
                        column[m] = column[m] + force[m][k : k + 8]
            contrib_force[pair + u] = jnp.zeros((8, A), jnp.float32)
            for m in range(3):
                contrib_force[pair + u, m : m + 1, :] = -jnp.sum(column[m], axis=0, keepdims=True)
        return carry

    lax.fori_loop(0, S // 2, backward, 0)
    for m in range(3):
        own_force[t, m : m + 1, :] = jnp.sum(jnp.transpose(own_acc[m]), axis=0, keepdims=True)


MESH = pl.DeviceIdType.MESH
PLANE = [(dy, dz) for dy in (-1, 0, 1) for dz in (-1, 0, 1) if (dy, dz) != (0, 0)]


def cell_of(dy, dz):
    return (dy + 1) * 3 + dz + 1


def step_kernel(
    nbr, counts, rates, pos, feat, mix, readout,
    forces, feature_grads,
    inverse, near_feat, near_pos, relay_feat, relay_pos,
    own, basis, stack, sums, inv, grad, gbuf, own_acc, own_force, contrib, contrib_force,
    feat_send, feat_recv, pos_send, pos_recv, *fold_refs,
):
    x, y, z = lax.axis_index("gx"), lax.axis_index("gy"), lax.axis_index("gz")
    ny, nz = lax.axis_size("gy"), lax.axis_size("gz")
    toward = 1 - 2 * lax.rem(x, 2)
    partner = (x + toward, y, z)
    has_far = (x - toward >= 0) & (x - toward < lax.axis_size("gx"))
    no_far = (x - toward < 0) | (x - toward >= lax.axis_size("gx"))
    pair_base = (toward + 1) * 9
    far_base = (1 - toward) * 9
    around = []
    for dy, dz in PLANE:
        exists = (y + dy >= 0) & (y + dy < ny) & (z + dz >= 0) & (z + dz < nz)
        around.append((dy, dz, (x, y + dy, z + dz), exists))

    place = jnp.where(x == 2, ny, 0) + y

    def ring(step):
        spot = lax.rem(place + step + 2 * ny, 2 * ny)
        side = spot // ny
        return (1 + side, lax.rem(spot, ny), z), (1 - side) * 18

    up, down = ring(1)[0], ring(-1)[0]
    (ahead, ahead_base), (behind, behind_base) = ring(ny - 1), ring(1 - ny)

    barrier = pltpu.get_barrier_semaphore()

    @pl.when(has_far)
    def _():
        for there in (ahead, behind):
            pl.semaphore_signal(barrier, inc=1, device_id=there, device_id_type=MESH)

        @pl.when(y == ny - 1)
        def _():
            pl.semaphore_signal(barrier, inc=1, device_id=up, device_id_type=MESH)

        @pl.when(y == 0)
        def _():
            pl.semaphore_signal(barrier, inc=1, device_id=down, device_id_type=MESH)

    for dy, dz, there, exists in around:
        @pl.when(exists)
        def _():
            pl.semaphore_signal(barrier, inc=1, device_id=there, device_id_type=MESH)

    pl.semaphore_signal(barrier, inc=1, device_id=partner, device_id_type=MESH)

    for t in range(T):
        valid = lax.broadcasted_iota(jnp.int32, (A, C), 0) < counts[t]
        near_feat[13 * T + t] = jnp.where(valid, feat[t].astype(jnp.float32), 0.0).astype(jnp.bfloat16)
    near_pos[13 * T : 14 * T] = pos[...]

    def clear(c):
        near_feat[pl.ds(c * T, T)] = jnp.zeros((T, A, C), jnp.bfloat16)
        near_pos[pl.ds(c * T, T)] = jnp.zeros((T, 3, A), jnp.float32)

    for dy, dz in PLANE:
        @pl.when((y + dy < 0) | (y + dy >= ny) | (z + dz < 0) | (z + dz >= nz))
        def _():
            for first in (0, 9, 18):
                clear(first + cell_of(dy, dz))

    @pl.when(no_far)
    def _():
        def one(c, carry):
            clear(far_base + c)
            return carry

        lax.fori_loop(0, 9, one, 0)

    def invert(n, carry):
        for t in range(T):
            found = jnp.int32(-1)
            for slot in range(S):
                found = jnp.where(nbr[t * S + slot] == n, slot, found)
            inverse[t * NEAR + n] = found
        return carry

    lax.fori_loop(0, NEAR, invert, 0)

    rows_near = 3 - jnp.where(y == 0, 1, 0) - jnp.where(y == ny - 1, 1, 0)
    columns_near = 3 - jnp.where(z == 0, 1, 0) - jnp.where(z == nz - 1, 1, 0)
    ring_peers = 2 + jnp.where(y == 0, 1, 0) + jnp.where(y == ny - 1, 1, 0)
    pl.semaphore_wait(barrier, rows_near * columns_near + jnp.where(has_far, ring_peers, 0))

    def send_tiles(feat_from, pos_from, feat_to, pos_to, k, there):
        return (
            pltpu.make_async_remote_copy(
                feat_from, feat_to, feat_send.at[k], feat_recv.at[k], device_id=there, device_id_type=MESH
            ),
            pltpu.make_async_remote_copy(
                pos_from, pos_to, pos_send.at[k], pos_recv.at[k], device_id=there, device_id_type=MESH
            ),
        )

    def send_rows(source, target, k, there):
        return send_tiles(near_feat.at[source], near_pos.at[source], near_feat.at[target], near_pos.at[target], k, there)

    def start(copies):
        for copy in copies:
            copy.start()

    def arrive(copies):
        for copy in copies:
            copy.wait_recv()

    def leave(copies):
        for copy in copies:
            copy.wait_send()

    def cells(cell):
        return pl.ds(cell * T, T)

    own_sends, far_sends, pair_sends = [], [[], []], []
    for k, (dy, dz, there, exists) in enumerate(around):
        own_sends.append(send_rows(cells(13), cells(9 + cell_of(-dy, -dz)), k, there))
        for t in range(T):
            target = pl.ds((far_base + cell_of(-dy, -dz)) * T + t, 1)
            far_sends[t].append(send_rows(pl.ds((far_base + 4) * T + t, 1), target, 8 + 8 * t + k, there))
        pair_sends.append(send_rows(cells(9 + cell_of(dy, dz)), cells(far_base + cell_of(dy, dz)), 24 + k, partner))
    centre_send = send_rows(cells(13), cells(far_base + 4), 32, partner)
    hops, relays = [], []
    for t, (first, last, last_base) in enumerate(((up, ahead, ahead_base), (down, behind, behind_base))):
        slot, source = pl.ds(t, 1), pl.ds(13 * T + t, 1)
        hops.append(
            send_tiles(near_feat.at[source], near_pos.at[source], relay_feat.at[slot], relay_pos.at[slot], 33 + t, first)
        )
        target = pl.ds((last_base + 4) * T + t, 1)
        relays.append(
            send_tiles(relay_feat.at[slot], relay_pos.at[slot], near_feat.at[target], near_pos.at[target], 35 + t, last)
        )

    @pl.when(has_far)
    def _():
        for t in range(T):
            start(hops[t])
        for t in range(T):
            arrive(hops[t])
            start(relays[t])

    for k in range(8):
        @pl.when(around[k][3])
        def _():
            start(own_sends[k])

    start(centre_send)
    for k in range(8):
        @pl.when(around[k][3])
        def _():
            arrive(own_sends[7 - k])
            start(pair_sends[k])

    for k in range(8):
        @pl.when(around[k][3])
        def _():
            arrive(pair_sends[k])

    arrive(centre_send)

    @pl.when(has_far)
    def _():
        for t in range(T):
            arrive(relays[t])
            for k in range(8):
                @pl.when(around[k][3])
                def _():
                    start(far_sends[t][k])
        for t in range(T):
            for k in range(8):
                @pl.when(around[k][3])
                def _():
                    arrive(far_sends[t][7 - k])

    def gradients(t, carry):
        tile_gradients(
            t, nbr, counts, rates, pos, near_pos, near_feat, mix, readout,
            own, basis, stack, sums, inv, grad, contrib,
        )
        return carry

    lax.fori_loop(0, T, gradients, 0)

    folds = [
        Fold(refs, source, inverse, around, (up, down), (ahead, behind), partner, (x, y, z), (ny, nz), (pair_base, far_base))
        for refs, source in ((fold_refs[:13], contrib), (fold_refs[13:], contrib_force))
    ]
    feature, push = folds

    def act(tile):
        tile_forces(tile, nbr, rates, near_pos, own, stack, grad, gbuf, own_acc, contrib_force, own_force)

    @pl.when(has_far)
    def _():
        feature.send_far_column()

    feature.send_pair_column()
    act(0)

    @pl.when(has_far)
    def _():
        feature.sum_far_column()

    act(1)

    @pl.when(has_far)
    def _():
        feature.relay()
        push.send_far_column()

    push.send_pair_column()
    feature.send_sides()

    @pl.when(has_far)
    def _():
        push.sum_far_column()

    push.send_sides()

    @pl.when(has_far)
    def _():
        push.relay()

    feature.send_rows()
    push.send_rows()
    feature.finish()
    push.finish()

    @pl.when(has_far)
    def _():
        push.finish_far()
        feature.finish_far()

    for t in range(T):
        valid = lax.broadcasted_iota(jnp.int32, (A, C), 0) < counts[t]
        feature_grads[t] = jnp.where(valid, feature.mid[1, t], 0.0)
        forces[t] = own_force[t] + push.mid[1, t, 0:3, :]

    @pl.when(has_far)
    def _():
        for t in range(T):
            leave(hops[t])
            leave(relays[t])
        for k in range(8):
            @pl.when(around[k][3])
            def _():
                for t in range(T):
                    leave(far_sends[t][k])

    for k in range(8):
        @pl.when(around[k][3])
        def _():
            leave(own_sends[k])
            leave(pair_sends[k])

    leave(centre_send)
    for fold in folds:
        fold.leave(has_far)


class Fold:
    def __init__(self, refs, source, inverse, around, near_ring, far_ring, partner, me, sizes, bases):
        (
            self.far_out, self.far_in, self.far_sum, self.passing, self.far_got,
            self.pair_out, self.pair_in, self.side_out, self.side_in, self.mid, self.row_in, send, recv,
        ) = refs
        self.source, self.inverse, self.around = source, inverse, around
        self.pair_base, self.far_base = bases
        (x, y, z), (ny, nz) = me, sizes

        def copy(from_ref, to_ref, k, there):
            return pltpu.make_async_remote_copy(
                from_ref, to_ref, send.at[k], recv.at[k], device_id=there, device_id_type=MESH
            )

        self.far = [copy(self.far_out.at[k], self.far_in.at[k], k, around[k][2]) for k in range(8)]
        self.pair = copy(self.pair_out, self.pair_in, 8, partner)
        self.side = [copy(self.side_out.at[d], self.side_in.at[d], 9 + d, (x, y, z + 2 * d - 1)) for d in range(2)]
        self.side_exists = [z > 0, z < nz - 1]
        self.row = [copy(self.mid.at[2 * d], self.row_in.at[d], 11 + d, (x, y + 2 * d - 1, z)) for d in range(2)]
        self.row_exists = [y > 0, y < ny - 1]
        self.hop = [copy(self.far_sum.at[t], self.passing.at[t], 13 + t, near_ring[t]) for t in range(T)]
        self.last = [copy(self.passing.at[t], self.far_got.at[t], 15 + t, far_ring[t]) for t in range(T)]

    def fill(self, ref, cell, extra=None):
        def one(u, carry):
            block = None
            for t in range(T):
                s = self.inverse[t * NEAR + cell * T + u]
                part = jnp.where(s >= 0, self.source[t * S + jnp.maximum(s, 0)], 0.0)
                block = part if block is None else block + part
            if extra is not None:
                block = block + extra[u]
            ref[u] = block
            return carry

        lax.fori_loop(0, T, one, 0)

    def send_far_column(self):
        for k, (dy, dz, there, exists) in enumerate(self.around):
            @pl.when(exists)
            def _():
                self.fill(self.far_out.at[k], self.far_base + cell_of(dy, dz))
                self.far[k].start()
        self.fill(self.far_sum, self.far_base + 4)

    def send_pair_column(self):
        def one(c, carry):
            self.fill(self.pair_out.at[c], self.pair_base + c)
            return carry

        lax.fori_loop(0, 9, one, 0)
        self.pair.start()

    def sum_far_column(self):
        for k in range(8):
            @pl.when(self.around[k][3])
            def _():
                self.far[7 - k].wait_recv()
                self.far_sum[...] += self.far_in[7 - k]
        for t in range(T):
            self.hop[t].start()

    def relay(self):
        for t in range(T):
            self.hop[t].wait_recv()
            self.last[t].start()

    def send_sides(self):
        self.pair.wait_recv()
        for d in range(2):
            @pl.when(self.side_exists[d])
            def _():
                for row in range(3):
                    c = row * 3 + 2 * d
                    self.fill(self.side_out.at[d, row], 9 + c, self.pair_in.at[c])
                self.side[d].start()
        for row in range(3):
            c = row * 3 + 1
            self.fill(self.mid.at[row], 9 + c, self.pair_in.at[c])

    def send_rows(self):
        for d in range(2):
            @pl.when(self.side_exists[d])
            def _():
                self.side[1 - d].wait_recv()
                for row in range(3):
                    self.mid[row] += self.side_in[1 - d, row]
        for d in range(2):
            @pl.when(self.row_exists[d])
            def _():
                self.row[d].start()

    def finish(self):
        for d in range(2):
            @pl.when(self.row_exists[d])
            def _():
                self.row[1 - d].wait_recv()
                self.mid[1] += self.row_in[1 - d]

    def finish_far(self):
        for t in range(T):
            self.last[t].wait_recv()
            self.mid[1, t] += self.far_got[t]

    def leave(self, has_far):
        @pl.when(has_far)
        def _():
            for k in range(8):
                @pl.when(self.around[k][3])
                def _():
                    self.far[k].wait_send()
            for t in range(T):
                self.hop[t].wait_send()
                self.last[t].wait_send()

        self.pair.wait_send()
        for d in range(2):
            @pl.when(self.side_exists[d])
            def _():
                self.side[d].wait_send()

            @pl.when(self.row_exists[d])
            def _():
                self.row[d].wait_send()


def fold_scratch(tile):
    shapes = [(8, T), (8, T), (T,), (T,), (T,), (9, T), (9, T), (2, 3, T), (2, 3, T), (3, T), (2, T)]
    return [pltpu.VMEM((*lead, *tile), jnp.float32) for lead in shapes] + [pltpu.SemaphoreType.DMA((17,))] * 2


def body(positions, features, counts, neighbours, mix_weight, readout, radial_rates):
    smem = pl.BlockSpec(memory_space=pltpu.SMEM)
    vmem = pl.BlockSpec(memory_space=pltpu.VMEM)
    forces, feature_grads = pl.pallas_call(
        step_kernel,
        out_shape=(
            jax.ShapeDtypeStruct((T, 3, A), jnp.float32),
            jax.ShapeDtypeStruct((T, A, C), jnp.float32),
        ),
        in_specs=[smem] * 3 + [vmem] * 4,
        out_specs=(vmem, vmem),
        scratch_shapes=[
            pltpu.SMEM((T * NEAR,), jnp.int32),
            pltpu.VMEM((NEAR, A, C), jnp.bfloat16),
            pltpu.VMEM((NEAR, 3, A), jnp.float32),
            pltpu.VMEM((T, A, C), jnp.bfloat16),
            pltpu.VMEM((T, 3, A), jnp.float32),
            pltpu.VMEM((T, 3, A, A), jnp.float32),
            pltpu.VMEM((T, 4 * R * A, S * A), jnp.bfloat16),
            pltpu.VMEM((T, S * A, C), jnp.bfloat16),
            pltpu.VMEM((4 * R * A, C), jnp.float32),
            pltpu.VMEM((A, 2 * R * C), jnp.bfloat16),
            pltpu.VMEM((T, 4 * R * A, C), jnp.bfloat16),
            pltpu.VMEM((4 * R * A, 2 * A), jnp.float32),
            pltpu.VMEM((3, A, A), jnp.float32),
            pltpu.VMEM((T, 3, A), jnp.float32),
            pltpu.VMEM((T * S, A, C), jnp.float32),
            pltpu.VMEM((T * S, 8, A), jnp.float32),
            pltpu.SemaphoreType.DMA((37,)),
            pltpu.SemaphoreType.DMA((37,)),
            pltpu.SemaphoreType.DMA((37,)),
            pltpu.SemaphoreType.DMA((37,)),
            *fold_scratch((A, C)),
            *fold_scratch((8, A)),
        ],
        compiler_params=pltpu.CompilerParams(
            collective_id=0, has_side_effects=True, vmem_limit_bytes=56 * 1024 * 1024
        ),
    )(
        neighbours.reshape(T * S), counts.reshape(T), radial_rates, positions.reshape(T, 3, A),
        features.reshape(T, A, C), mix_weight, readout.reshape(1, C),
    )
    return (
        forces.reshape(1, 1, 1, T, 3, A),
        feature_grads.reshape(1, 1, 1, T, A, C),
    )


def solution(mesh):
    cell = ("gx", "gy", "gz")
    in_specs = (
        P(*cell, None, None, None),
        P(*cell, None, None, None),
        P(*cell, None),
        P(*cell, None, None),
        P(),
        P(),
        P(),
    )
    out_specs = (P(*cell, None, None, None), P(*cell, None, None, None))
    return jax.shard_map(body, mesh=mesh, in_specs=in_specs, out_specs=out_specs, check_vma=False)
```

```python
import functools

import jax
import jax.numpy as jnp
from jax import lax
from jax.experimental import pallas as pl
from jax.experimental.pallas import tpu as pltpu
from jax.sharding import PartitionSpec as P

A = 128
C = 128
R = 4
S = 8
T = 2
NEAR = 27 * T
ROWS = 136
SCALING = (S * A) ** -0.5
CHUNK = 32


def pair_geometry(near, own, t, base, size):
    offset = [near[m : m + 1, :] - own[t, m, pl.ds(base, size), :] for m in range(3)]
    square = offset[0] * offset[0] + offset[1] * offset[1] + offset[2] * offset[2]
    return offset, square


def tile_basis(t, nbr, rates, pos, near_pos, own, basis):
    for m in range(3):
        own[t, m] = jnp.transpose(jnp.broadcast_to(pos[t, m : m + 1, :], (A, A)))

    def build(s, carry):
        n = nbr[t * S + s]
        source = jnp.maximum(n, 0)
        near = near_pos[source]
        lanes = pl.ds(pl.multiple_of(s * A, A), A)
        for base in range(0, A, CHUNK):
            offset, square = pair_geometry(near, own, t, base, CHUNK)
            for r in range(R):
                g = jnp.exp(-rates[r] * square)
                for m in range(4):
                    value = g if m == 0 else g * offset[m - 1]
                    row = (r * 4 + m) * A + base
                    basis[t, row : row + CHUNK, lanes] = value.astype(jnp.bfloat16)
        return carry

    lax.fori_loop(0, S, build, 0)


def tile_gradients(t, nbr, counts, near_feat, mix, readout, basis, stack, sums, inv, grad, contrib):
    for s in range(S):
        n = nbr[t * S + s]
        tile = near_feat[jnp.maximum(n, 0)]
        stack[t, s * A : (s + 1) * A, :] = jnp.where(n >= 0, tile, jnp.zeros_like(tile))

    def forward(k, carry):
        rows = pl.ds(pl.multiple_of(k * 4 * A, 4 * A), 4 * A)
        sums[rows, :] = jnp.dot(basis[t, rows, :], stack[t], preferred_element_type=jnp.float32) * SCALING
        return carry

    lax.fori_loop(0, R, forward, 0)

    for r in range(R):
        base = r * 4 * A
        inv[:, r * C : (r + 1) * C] = sums[base : base + A, :].astype(jnp.bfloat16)
        total = jnp.zeros((A, C), jnp.float32)
        for m in range(1, 4):
            part = sums[base + m * A : base + (m + 1) * A, :]
            total = total + part * part
        inv[:, (R + r) * C : (R + r + 1) * C] = total.astype(jnp.bfloat16)
    preact = jnp.dot(inv[...], mix[...], preferred_element_type=jnp.float32)
    sigmoid = 1.0 / (1.0 + jnp.exp(-preact))
    valid = lax.broadcasted_iota(jnp.int32, (A, C), 0) < counts[t]
    grad_pre = readout[...] * sigmoid * (1.0 + preact * (1.0 - sigmoid))
    grad_pre = jnp.where(valid, grad_pre, 0.0).astype(jnp.bfloat16)
    for r in range(R):
        base = r * 4 * A
        for half in range(2):
            k = half * R + r
            gi = lax.dot_general(
                grad_pre, mix[k * C : (k + 1) * C, :], (((1,), (1,)), ((), ())),
                preferred_element_type=jnp.float32,
            )
            if half == 0:
                grad[t, base : base + A, :] = (gi * SCALING).astype(jnp.bfloat16)
            else:
                for m in range(1, 4):
                    rows = slice(base + m * A, base + (m + 1) * A)
                    grad[t, rows, :] = (2.0 * sums[rows, :] * gi * SCALING).astype(jnp.bfloat16)

    def spread(p, carry):
        wide = pl.ds(pl.multiple_of(p * 2 * A, 2 * A), 2 * A)
        near_grad = lax.dot_general(
            basis[t, :, wide], grad[t], (((0,), (0,)), ((), ())), preferred_element_type=jnp.float32
        )
        pair = t * S + p * 2
        contrib[pair] = near_grad[:A]
        contrib[pair + 1] = near_grad[A:]
        return carry

    lax.fori_loop(0, S // 2, spread, 0)


def tile_forces(t, nbr, rates, near_pos, own, stack, grad, gbuf, own_acc, contrib_force, own_force):
    for m in range(3):
        own_acc[m] = jnp.zeros((A, A), jnp.float32)

    def backward(p, carry):
        wide = pl.ds(pl.multiple_of(p * 2 * A, 2 * A), 2 * A)
        pair = t * S + p * 2
        gbuf[...] = lax.dot_general(
            grad[t], stack[t, wide, :], (((1,), (1,)), ((), ())), preferred_element_type=jnp.float32
        )
        for u in range(2):
            near = near_pos[jnp.maximum(nbr[pair + u], 0)]
            cols = slice(u * A, (u + 1) * A)
            column = [jnp.zeros((8, A), jnp.float32) for _ in range(3)]
            for base in range(0, A, CHUNK):
                offset, square = pair_geometry(near, own, t, base, CHUNK)
                force = [None] * 3
                pull = None
                for r in range(R):
                    g = jnp.exp(-rates[r] * square)
                    gb = [gbuf[(r * 4 + m) * A + base : (r * 4 + m) * A + base + CHUNK, cols] for m in range(4)]
                    inner = gb[0] + gb[1] * offset[0] + gb[2] * offset[1] + gb[3] * offset[2]
                    term = (2.0 * rates[r]) * g * inner
                    pull = term if pull is None else pull + term
                    for m in range(3):
                        part = g * gb[m + 1]
                        force[m] = part if force[m] is None else force[m] + part
                for m in range(3):
                    force[m] = force[m] - offset[m] * pull
                    own_acc[m, base : base + CHUNK, :] += force[m]
                    for k in range(0, CHUNK, 8):
                        column[m] = column[m] + force[m][k : k + 8]
            contrib_force[pair + u] = jnp.zeros((8, A), jnp.float32)
            for m in range(3):
                contrib_force[pair + u, m : m + 1, :] = -jnp.sum(column[m], axis=0, keepdims=True)
        return carry

    lax.fori_loop(0, S // 2, backward, 0)
    for m in range(3):
        own_force[t, m : m + 1, :] = jnp.sum(jnp.transpose(own_acc[m]), axis=0, keepdims=True)


MESH = pl.DeviceIdType.MESH
PLANE = [(dy, dz) for dy in (-1, 0, 1) for dz in (-1, 0, 1) if (dy, dz) != (0, 0)]


def cell_of(dy, dz):
    return (dy + 1) * 3 + dz + 1


def step_kernel(
    nbr, counts, rates, pos, feat, mix, readout,
    forces, feature_grads,
    inverse, near_feat, near_pos,
    own, basis, stack, sums, inv, grad, gbuf, own_acc, own_force, contrib, contrib_force,
    feat_send, feat_recv, pos_send, pos_recv, *fold_refs,
):
    x, y, z = lax.axis_index("gx"), lax.axis_index("gy"), lax.axis_index("gz")
    ny, nz = lax.axis_size("gy"), lax.axis_size("gz")
    toward = 1 - 2 * lax.rem(x, 2)
    partner = (x + toward, y, z)
    has_far = (x - toward >= 0) & (x - toward < lax.axis_size("gx"))
    no_far = (x - toward < 0) | (x - toward >= lax.axis_size("gx"))
    pair_base = (toward + 1) * 9
    far_base = (1 - toward) * 9
    around = []
    for dy, dz in PLANE:
        exists = (y + dy >= 0) & (y + dy < ny) & (z + dz >= 0) & (z + dz < nz)
        around.append((dy, dz, (x, y + dy, z + dz), exists))

    across = (x - toward, y, z)

    barrier = pltpu.get_barrier_semaphore()

    @pl.when(has_far)
    def _():
        pl.semaphore_signal(barrier, inc=1, device_id=across, device_id_type=MESH)

    for dy, dz, there, exists in around:
        @pl.when(exists)
        def _():
            pl.semaphore_signal(barrier, inc=1, device_id=there, device_id_type=MESH)

    pl.semaphore_signal(barrier, inc=1, device_id=partner, device_id_type=MESH)

    for t in range(T):
        valid = lax.broadcasted_iota(jnp.int32, (A, C), 0) < counts[t]
        near_feat[13 * T + t] = jnp.where(valid, feat[t].astype(jnp.float32), 0.0).astype(jnp.bfloat16)
    near_pos[13 * T : 14 * T] = pos[...]

    def clear(c):
        near_feat[pl.ds(c * T, T)] = jnp.zeros((T, A, C), jnp.bfloat16)
        near_pos[pl.ds(c * T, T)] = jnp.zeros((T, 3, A), jnp.float32)

    for dy, dz in PLANE:
        @pl.when((y + dy < 0) | (y + dy >= ny) | (z + dz < 0) | (z + dz >= nz))
        def _():
            for first in (0, 9, 18):
                clear(first + cell_of(dy, dz))

    @pl.when(no_far)
    def _():
        def one(c, carry):
            clear(far_base + c)
            return carry

        lax.fori_loop(0, 9, one, 0)

    def invert(n, carry):
        for t in range(T):
            found = jnp.int32(-1)
            for slot in range(S):
                found = jnp.where(nbr[t * S + slot] == n, slot, found)
            inverse[t * NEAR + n] = found
        return carry

    lax.fori_loop(0, NEAR, invert, 0)

    rows_near = 3 - jnp.where(y == 0, 1, 0) - jnp.where(y == ny - 1, 1, 0)
    columns_near = 3 - jnp.where(z == 0, 1, 0) - jnp.where(z == nz - 1, 1, 0)
    pl.semaphore_wait(barrier, rows_near * columns_near + jnp.where(has_far, 1, 0))

    def send_tiles(feat_from, pos_from, feat_to, pos_to, k, there):
        return (
            pltpu.make_async_remote_copy(
                feat_from, feat_to, feat_send.at[k], feat_recv.at[k], device_id=there, device_id_type=MESH
            ),
            pltpu.make_async_remote_copy(
                pos_from, pos_to, pos_send.at[k], pos_recv.at[k], device_id=there, device_id_type=MESH
            ),
        )

    def send_rows(source, target, k, there):
        return send_tiles(near_feat.at[source], near_pos.at[source], near_feat.at[target], near_pos.at[target], k, there)

    def leave(copies):
        for copy in copies:
            copy.wait_send()

    def cells(cell):
        return pl.ds(cell * T, T)

    own_sends, far_sends, pair_sends = [], [[], []], []
    for k, (dy, dz, there, exists) in enumerate(around):
        own_sends.append(send_rows(cells(13), cells(9 + cell_of(-dy, -dz)), k, there))
        for t in range(T):
            target = pl.ds((far_base + cell_of(-dy, -dz)) * T + t, 1)
            far_sends[t].append(send_rows(pl.ds((far_base + 4) * T + t, 1), target, 8 + 8 * t + k, there))
        pair_sends.append(send_rows(cells(9 + cell_of(dy, dz)), cells(far_base + cell_of(dy, dz)), 24 + k, partner))
    centre_send = send_rows(cells(13), cells(far_base + 4), 32, partner)
    crossing = [
        send_rows(pl.ds(13 * T + t, 1), pl.ds((pair_base + 4) * T + t, 1), 33 + t, across) for t in range(T)
    ]

    for kind in (1, 0):
        @pl.when(has_far)
        def _():
            for t in range(T):
                crossing[t][kind].start()

        for k in range(8):
            @pl.when(around[k][3])
            def _():
                own_sends[k][kind].start()

        centre_send[kind].start()

    for kind in (1, 0):
        for k in range(8):
            @pl.when(around[k][3])
            def _():
                own_sends[7 - k][kind].wait_recv()
                pair_sends[k][kind].start()

    def receive(kind):
        @pl.when(has_far)
        def _():
            for t in range(T):
                crossing[t][kind].wait_recv()
                for k in range(8):
                    @pl.when(around[k][3])
                    def _():
                        far_sends[t][k][kind].start()

        for k in range(8):
            @pl.when(around[k][3])
            def _():
                pair_sends[k][kind].wait_recv()

        centre_send[kind].wait_recv()

        @pl.when(has_far)
        def _():
            for t in range(T):
                for k in range(8):
                    @pl.when(around[k][3])
                    def _():
                        far_sends[t][7 - k][kind].wait_recv()

    receive(1)

    def expand(t, carry):
        tile_basis(t, nbr, rates, pos, near_pos, own, basis)
        return carry

    lax.fori_loop(0, T, expand, 0)
    receive(0)

    def gradients(t, carry):
        tile_gradients(t, nbr, counts, near_feat, mix, readout, basis, stack, sums, inv, grad, contrib)
        return carry

    lax.fori_loop(0, T, gradients, 0)

    folds = [
        Fold(refs, source, inverse, around, across, partner, (x, y, z), (ny, nz), (pair_base, far_base))
        for refs, source in ((fold_refs[:16], contrib), (fold_refs[16:], contrib_force))
    ]
    feature, push = folds

    def act(tile):
        tile_forces(tile, nbr, rates, near_pos, own, stack, grad, gbuf, own_acc, contrib_force, own_force)

    @pl.when(has_far)
    def _():
        feature.send_far_column()

    feature.send_pair_column()
    act(0)

    @pl.when(has_far)
    def _():
        feature.sum_far_column()

    act(1)

    @pl.when(has_far)
    def _():
        push.send_far_column()

    push.send_pair_column()
    feature.send_sides()

    @pl.when(has_far)
    def _():
        push.sum_far_column()

    push.send_sides()

    feature.send_rows()
    push.send_rows()
    feature.finish()
    push.finish()

    @pl.when(has_far)
    def _():
        push.finish_far()
        feature.finish_far()

    for t in range(T):
        valid = lax.broadcasted_iota(jnp.int32, (A, C), 0) < counts[t]
        feature_grads[t] = jnp.where(valid, feature.mid[1, t], 0.0)
        forces[t] = own_force[t] + push.mid[1, t, 0:3, :]

    @pl.when(has_far)
    def _():
        for t in range(T):
            leave(crossing[t])
        for k in range(8):
            @pl.when(around[k][3])
            def _():
                for t in range(T):
                    leave(far_sends[t][k])

    for k in range(8):
        @pl.when(around[k][3])
        def _():
            leave(own_sends[k])
            leave(pair_sends[k])

    leave(centre_send)
    for fold in folds:
        fold.leave(has_far)


class Fold:
    def __init__(self, refs, source, inverse, around, across, partner, me, sizes, bases):
        (
            self.far_out, self.far_in, self.far_sum, self.far_got,
            self.pair_out, self.pair_in, self.side_out, self.side_in, self.mid, self.row_in, send, recv, *self.coded
        ) = refs
        self.source, self.inverse, self.around = source, inverse, around
        self.pair_base, self.far_base = bases
        (x, y, z), (ny, nz) = me, sizes

        def copy(from_ref, to_ref, k, there):
            return pltpu.make_async_remote_copy(
                from_ref, to_ref, send.at[k], recv.at[k], device_id=there, device_id_type=MESH
            )

        self.far = [copy(self.far_out.at[k], self.far_in.at[k], k, around[k][2]) for k in range(8)]
        self.pair = copy(self.pair_out, self.pair_in, 8, partner)
        self.side = [copy(self.side_out.at[d], self.side_in.at[d], 9 + d, (x, y, z + 2 * d - 1)) for d in range(2)]
        self.side_exists = [z > 0, z < nz - 1]
        self.row = [copy(self.mid.at[2 * d], self.row_in.at[d], 11 + d, (x, y + 2 * d - 1, z)) for d in range(2)]
        self.row_exists = [y > 0, y < ny - 1]
        if self.coded:
            code_out, code_in, step_out, step_in = self.coded
            self.cross = [copy(step_out, step_in, 13, across), copy(code_out, code_in, 14, across)]
        else:
            self.cross = [copy(self.far_sum, self.far_got, 13, across)]

    def fill(self, ref, cell, extra=None):
        def one(u, carry):
            block = None
            for t in range(T):
                s = self.inverse[t * NEAR + cell * T + u]
                part = jnp.where(s >= 0, self.source[t * S + jnp.maximum(s, 0)], 0.0)
                block = part if block is None else block + part
            if extra is not None:
                block = block + extra[u]
            ref[u] = block
            return carry

        lax.fori_loop(0, T, one, 0)

    def send_far_column(self):
        for k, (dy, dz, there, exists) in enumerate(self.around):
            @pl.when(exists)
            def _():
                self.fill(self.far_out.at[k], self.far_base + cell_of(dy, dz))
                self.far[k].start()
        self.fill(self.far_sum, self.far_base + 4)

    def send_pair_column(self):
        def one(c, carry):
            self.fill(self.pair_out.at[c], self.pair_base + c)
            return carry

        lax.fori_loop(0, 9, one, 0)
        self.pair.start()

    def sum_far_column(self):
        for k in range(8):
            @pl.when(self.around[k][3])
            def _():
                self.far[7 - k].wait_recv()
                self.far_sum[...] += self.far_in[7 - k]
        if self.coded:
            self.encode()
        for part in self.cross:
            part.start()

    def encode(self):
        code_out, _, step_out, _ = self.coded
        for t in range(T):
            block = self.far_sum[t]
            largest = jnp.maximum(jnp.max(jnp.abs(block), axis=0, keepdims=True), 1e-30)
            step_out[t] = jnp.broadcast_to(largest * (1.0 / 32767.0), (8, C))
            code = (block * (32767.0 / largest) + 32768.5).astype(jnp.int32) - 32768
            code_out[t] = code.astype(jnp.int16)

    def send_sides(self):
        self.pair.wait_recv()
        for d in range(2):
            @pl.when(self.side_exists[d])
            def _():
                for row in range(3):
                    c = row * 3 + 2 * d
                    self.fill(self.side_out.at[d, row], 9 + c, self.pair_in.at[c])
                self.side[d].start()
        for row in range(3):
            c = row * 3 + 1
            self.fill(self.mid.at[row], 9 + c, self.pair_in.at[c])

    def send_rows(self):
        for d in range(2):
            @pl.when(self.side_exists[d])
            def _():
                self.side[1 - d].wait_recv()
                for row in range(3):
                    self.mid[row] += self.side_in[1 - d, row]
        for d in range(2):
            @pl.when(self.row_exists[d])
            def _():
                self.row[d].start()

    def finish(self):
        for d in range(2):
            @pl.when(self.row_exists[d])
            def _():
                self.row[1 - d].wait_recv()
                self.mid[1] += self.row_in[1 - d]

    def finish_far(self):
        for part in self.cross:
            part.wait_recv()
        for t in range(T):
            if self.coded:
                _, code_in, _, step_in = self.coded
                got = code_in[t].astype(jnp.int32).astype(jnp.float32) * step_in[t, 0:1, :]
            else:
                got = self.far_got[t]
            self.mid[1, t] += got

    def leave(self, has_far):
        @pl.when(has_far)
        def _():
            for k in range(8):
                @pl.when(self.around[k][3])
                def _():
                    self.far[k].wait_send()
            for part in self.cross:
                part.wait_send()

        self.pair.wait_send()
        for d in range(2):
            @pl.when(self.side_exists[d])
            def _():
                self.side[d].wait_send()

            @pl.when(self.row_exists[d])
            def _():
                self.row[d].wait_send()


def fold_scratch(tile):
    shapes = [(8, T), (8, T), (T,), (T,), (9, T), (9, T), (2, 3, T), (2, 3, T), (3, T), (2, T)]
    return [pltpu.VMEM((*lead, *tile), jnp.float32) for lead in shapes] + [pltpu.SemaphoreType.DMA((15,))] * 2


def body(positions, features, counts, neighbours, mix_weight, readout, radial_rates):
    smem = pl.BlockSpec(memory_space=pltpu.SMEM)
    vmem = pl.BlockSpec(memory_space=pltpu.VMEM)
    forces, feature_grads = pl.pallas_call(
        step_kernel,
        out_shape=(
            jax.ShapeDtypeStruct((T, 3, A), jnp.float32),
            jax.ShapeDtypeStruct((T, A, C), jnp.float32),
        ),
        in_specs=[smem] * 3 + [vmem] * 4,
        out_specs=(vmem, vmem),
        scratch_shapes=[
            pltpu.SMEM((T * NEAR,), jnp.int32),
            pltpu.VMEM((NEAR, A, C), jnp.bfloat16),
            pltpu.VMEM((NEAR, 3, A), jnp.float32),
            pltpu.VMEM((T, 3, A, A), jnp.float32),
            pltpu.VMEM((T, 4 * R * A, S * A), jnp.bfloat16),
            pltpu.VMEM((T, S * A, C), jnp.bfloat16),
            pltpu.VMEM((4 * R * A, C), jnp.float32),
            pltpu.VMEM((A, 2 * R * C), jnp.bfloat16),
            pltpu.VMEM((T, 4 * R * A, C), jnp.bfloat16),
            pltpu.VMEM((4 * R * A, 2 * A), jnp.float32),
            pltpu.VMEM((3, A, A), jnp.float32),
            pltpu.VMEM((T, 3, A), jnp.float32),
            pltpu.VMEM((T * S, A, C), jnp.float32),
            pltpu.VMEM((T * S, 8, A), jnp.float32),
            pltpu.SemaphoreType.DMA((35,)),
            pltpu.SemaphoreType.DMA((35,)),
            pltpu.SemaphoreType.DMA((35,)),
            pltpu.SemaphoreType.DMA((35,)),
            *fold_scratch((A, C)),
            pltpu.VMEM((T, A, C), jnp.int16),
            pltpu.VMEM((T, A, C), jnp.int16),
            pltpu.VMEM((T, 8, C), jnp.float32),
            pltpu.VMEM((T, 8, C), jnp.float32),
            *fold_scratch((8, A)),
        ],
        compiler_params=pltpu.CompilerParams(
            collective_id=0, has_side_effects=True, vmem_limit_bytes=56 * 1024 * 1024
        ),
    )(
        neighbours.reshape(T * S), counts.reshape(T), radial_rates, positions.reshape(T, 3, A),
        features.reshape(T, A, C), mix_weight, readout.reshape(1, C),
    )
    return (
        forces.reshape(1, 1, 1, T, 3, A),
        feature_grads.reshape(1, 1, 1, T, A, C),
    )


def solution(mesh):
    cell = ("gx", "gy", "gz")
    in_specs = (
        P(*cell, None, None, None),
        P(*cell, None, None, None),
        P(*cell, None),
        P(*cell, None, None),
        P(),
        P(),
        P(),
    )
    out_specs = (P(*cell, None, None, None), P(*cell, None, None, None))
    return jax.shard_map(body, mesh=mesh, in_specs=in_specs, out_specs=out_specs, check_vma=False)
```
